32 devices in a mesh: ctx: 8 (over y, x, core), head: 4 (over z).
Axes of the slice: x: 2, y: 2, z: 4, core: 2. Of those that a mesh axis runs over, the one named last changes fastest.
Arguments:
- query: bfloat16 [1024, 24576], P('ctx', 'head'), may hold values from -8 to 8
- latent: bfloat16 [1024, 576], P(('ctx', 'head')), may hold values from -8 to 8
- w_key_up: bfloat16 [512, 16384], P(None, 'head'), may hold values from -0.25 to 0.25
- w_value_up: bfloat16 [512, 16384], P(None, 'head'), may hold values from -0.25 to 0.25
- cotangent: bfloat16 [1024, 16384], P('ctx', 'head'), may hold values from -6 to 6
- window_start: int32 [8], P('ctx'), may hold values from 0 to 703, as said below
Outputs:
- attn_out: bfloat16 [1024, 16384], P('ctx', 'head')
- query_grad: bfloat16 [1024, 24576], P('ctx', 'head')
- latent_grad: float32 [1024, 576], P(('ctx', 'head'))
- key_up_grad: float32 [512, 16384], P('ctx', 'head')
- value_up_grad: float32 [512, 16384], P('ctx', 'head')
The draws below stay inside these ranges and needn't reach their ends.
Inputs may be any that keep to these rules, and one draw needn't show every extreme that they name: window_start[b] is at least max(0, (b - 2) * 128) and less than max(1, (b - 2) * 128 + 128 // 2).
All inputs are finite; a program needn't handle non-finite values.
Results may differ from the reference program's by a relative error of at most 0.0099.
Values may be sent and summed in bfloat16 or wider, within the bound.
No kernel may reach another device: no remote copies, remote signals or barrier semaphores. Data moves between devices by JAX's collectives and lax.ppermute only.
A program may use at most 128 MiB of HBM per device.

```python
import jax
import jax.numpy as jnp
from jax import lax

H = 128
LAT = 512
ROPE = 64
NOPE = 128
VD = 128
TD = 128
KB = 2
TOKENS = 1024
NBLK = 8


def draw_query(key, part):
    first = jax.random.fold_in(key, 1)
    base = jax.random.truncated_normal(first, -6.0, 6.0, (TOKENS, H, NOPE + ROPE), jnp.float32)
    return base.reshape(TOKENS, H * (NOPE + ROPE)).astype(jnp.bfloat16)


def draw_latent(key, part):
    first = jax.random.fold_in(key, 3)
    base = jax.random.truncated_normal(first, -6.0, 6.0, (TOKENS, LAT + ROPE), jnp.float32)
    return base.astype(jnp.bfloat16)


def draw_window_start(key, part):
    blocks = jnp.arange(TOKENS // TD, dtype=jnp.int32)
    jitter = jax.random.randint(jax.random.fold_in(key, 5), (TOKENS // TD,), 0, TD // 2)
    return jnp.maximum(0, (blocks - KB) * TD + jitter).astype(jnp.int32)


def block_scale(stream_key, shape, pieces, low, largest):
    def one(axis_at, parts):
        draws = jax.random.uniform(jax.random.fold_in(jax.random.fold_in(stream_key, 6), axis_at), (parts,), jnp.float32, low / len(pieces), largest / len(pieces))
        return jnp.repeat(jnp.exp(draws), shape[axis_at] // parts).reshape((-1,) + (1,) * (len(shape) - axis_at - 1))

    factor_of = one(*pieces[0])
    for cut in pieces[1:]:
        factor_of = factor_of * one(*cut)
    return factor_of


def noise(key, shape, deviation, bound, cuts=(), kind=jnp.bfloat16):
    gain = block_scale(key, shape, cuts, -0.22, 0.18) if cuts else 1.0
    result = jax.random.normal(key, shape, jnp.float32) * deviation * gain
    return jnp.minimum(jnp.maximum(result, -bound), bound).astype(kind)


def setup_inputs(seed: int = 0) -> dict:
    seeds = jax.random.split(jax.random.key(seed), 7)
    return {
        "query": draw_query(jax.random.fold_in(seeds[6], 71), 0),
        "latent": draw_latent(jax.random.fold_in(seeds[6], 71), 0),
        "w_key_up": noise(seeds[2], (LAT, H * NOPE), LAT ** -0.5, 0.25, ((1, 4),)),
        "w_value_up": noise(seeds[3], (LAT, H * VD), LAT ** -0.5, 0.25, ((1, 4),)),
        "cotangent": noise(seeds[4], (TOKENS, H * VD), 1.0, 6.0, ((0, 8), (1, 4))),
        "window_start": draw_window_start(jax.random.fold_in(seeds[6], 71), 0),
    }


def rounded(value):
    return lax.optimization_barrier(value.astype(jnp.bfloat16)).astype(jnp.float32)


def product(form, left, right):
    return jnp.einsum(form, left.astype(jnp.float32), right.astype(jnp.float32), precision=lax.Precision.HIGHEST)


def reference(query, latent, w_key_up, w_value_up, cotangent, window_start):
    scale = (NOPE + ROPE) ** -0.5
    span = (KB + 1) * TD
    w_key = w_key_up.astype(jnp.float32).reshape(LAT, H, NOPE)
    w_value = w_value_up.astype(jnp.float32).reshape(LAT, H, VD)
    padded = jnp.concatenate([jnp.zeros((KB * TD, LAT + ROPE), jnp.float32), latent.astype(jnp.float32)], 0)

    def block(carry, index):
        grads, key_acc, value_acc = carry
        begin = (index * TD).astype(jnp.int32)
        window = lax.dynamic_slice_in_dim(padded, begin, span, 0)
        queries = lax.dynamic_slice_in_dim(query, begin, TD, 0).astype(jnp.float32).reshape(TD, H, NOPE + ROPE)
        q_nope = queries[..., :NOPE]
        q_rope = queries[..., NOPE:]
        grad_out = lax.dynamic_slice_in_dim(cotangent, begin, TD, 0).astype(jnp.float32).reshape(TD, H, VD)
        absorbed = rounded(product('thd,lhd->thl', q_nope, w_key))
        q_full = jnp.concatenate([absorbed, q_rope], -1)
        scores = product('thc,kc->htk', q_full, window) * scale
        q_pos = begin + jnp.arange(TD, dtype=jnp.int32)
        k_pos = begin - KB * TD + jnp.arange(span, dtype=jnp.int32)
        allowed = (k_pos[None, :] >= window_start[index]) & (k_pos[None, :] <= q_pos[:, None])
        scores = jnp.where(allowed[None], scores, -1e30)
        top = jnp.max(scores, -1, keepdims=True)
        expo = jnp.where(allowed[None], jnp.exp(scores - top), 0.0)
        probs = expo / jnp.sum(expo, -1, keepdims=True)
        probs_b = rounded(probs)
        mixed = rounded(product('htk,kc->thc', probs_b, window[:, :LAT]))
        out_full = product('thc,chv->thv', mixed, w_value)
        grad_absorbed = rounded(product('thv,chv->thc', grad_out, w_value))
        dprobs = product('thc,kc->htk', grad_absorbed, window[:, :LAT])
        delta = jnp.sum(grad_out * out_full, -1).T[:, :, None]
        dscores = rounded(probs * (dprobs - delta) * scale)
        attended = rounded(product('htk,kc->thc', dscores, window))
        dq_nope = product('thc,chd->thd', attended[..., :LAT], w_key)
        dq = jnp.concatenate([dq_nope, attended[..., LAT:]], -1).astype(jnp.bfloat16).reshape(TD, H * (NOPE + ROPE))
        value_side = product('htk,thc->kc', probs_b, grad_absorbed)
        lat_part = product('htk,thc->kc', dscores, q_full) + jnp.concatenate([value_side, jnp.zeros((span, ROPE), jnp.float32)], -1)
        old = lax.dynamic_slice_in_dim(grads, begin, span, 0)
        grads = lax.dynamic_update_slice_in_dim(grads, old + lat_part, begin, 0)
        key_acc = key_acc + product('thc,thd->chd', attended[..., :LAT], q_nope)
        value_acc = value_acc + product('thc,thv->chv', mixed, grad_out)
        out = out_full.astype(jnp.bfloat16).reshape(TD, H * VD)
        return (grads, key_acc, value_acc), (out, dq)

    start = (jnp.zeros((TOKENS + KB * TD, LAT + ROPE), jnp.float32), jnp.zeros((LAT, H, NOPE), jnp.float32), jnp.zeros((LAT, H, VD), jnp.float32))
    (grads, key_acc, value_acc), (outs, dqs) = lax.scan(block, start, jnp.arange(NBLK, dtype=jnp.int32))
    attn_out = outs.reshape(TOKENS, H * VD)
    query_grad = dqs.reshape(TOKENS, H * (NOPE + ROPE))
    latent_grad = grads[KB * TD:]
    return attn_out, query_grad, latent_grad, key_acc.reshape(LAT, H * NOPE), value_acc.reshape(LAT, H * VD)
```

```python
import functools

import jax
import jax.numpy as jnp
from jax import lax
from jax.experimental import pallas as pl
from jax.experimental.pallas import tpu as pltpu
from jax.sharding import PartitionSpec as P

LAT = 512
ROPE = 64
NOPE = 128
VD = 128
HD = NOPE + ROPE
KB = 2
CHUNKS = 4

BF = jnp.bfloat16
F32 = jnp.float32
NT = (((1,), (1,)), ((), ()))


def dot(a, b):
    return jnp.dot(a, b, preferred_element_type=F32)


def dot_nt(a, b):
    return lax.dot_general(a, b, NT, preferred_element_type=F32)


def bits_of(n):
    return n.bit_length() - 1


def swap(x, axis, flip):
    n = lax.axis_size(axis)
    return lax.ppermute(x, axis, [(i, i ^ flip) for i in range(n)])


def shifted(block, axis, distance):
    devices = range(lax.axis_size(axis))
    route = [(i - distance, i) for i in devices if i - distance in devices]
    return lax.ppermute(block, axis, route)


def slot_masks(order):
    n = 1 << len(order)
    masks = []
    for k in range(n):
        mask = 0
        for i, p in enumerate(order):
            if (k >> (len(order) - 1 - i)) & 1:
                mask |= 1 << p
        masks.append(mask)
    return masks


def body(masks, shard, n_in, meta, q_ref, wk_ref, wv_ref, g_ref, win_ref, lat_in, *rest):
    attn_ref, qg_ref, lat_ref, keep_ref, send_ref = rest[n_in : n_in + 5]
    win_t, bias, qf, ga, qd, gd, buf = rest[n_in + 5 :]
    span = win_ref.shape[0]
    rows = q_ref.shape[0]
    scale = HD ** (-0.5)

    @pl.when(pl.program_id(0) == 0)
    def _():
        win_t[...] = win_ref[...].T
        lat_ref[...] = lat_in[...]
        qd[...] = jnp.zeros_like(qd)
        gd[...] = jnp.zeros_like(gd)
        k = lax.broadcasted_iota(jnp.int32, (span, 2 * rows), 0)
        t = lax.broadcasted_iota(jnp.int32, (span, 2 * rows), 1) & (rows - 1)
        pos = k ^ (meta[1] * shard)
        allowed = (pos >= meta[0]) & (pos <= t + (span - rows))
        bias[...] = jnp.where(allowed, 0.0, -1e30).astype(F32)

    q = q_ref[...]
    g = g_ref[...]
    for h in range(2):
        at = slice(h * rows, (h + 1) * rows)
        q_nope = q[:, h * HD : h * HD + NOPE]
        g_h = g[:, h * VD : (h + 1) * VD]
        qf[at, :LAT] = dot_nt(q_nope, wk_ref[:, h * NOPE : (h + 1) * NOPE]).astype(BF)
        qf[at, LAT:] = q[:, h * HD + NOPE : (h + 1) * HD]
        ga[at, :] = dot_nt(g_h, wv_ref[:, h * VD : (h + 1) * VD]).astype(BF)
        qd[at, h * NOPE : (h + 1) * NOPE] = q_nope
        gd[at, h * VD : (h + 1) * VD] = g_h
    s = dot_nt(win_ref[...], qf[...]) * scale + bias[...]
    e = jnp.exp(s - jnp.max(s, 0, keepdims=True))
    p = e * (1.0 / jnp.sum(e, 0, keepdims=True))
    pb = p.astype(BF)
    mix = dot(win_t[:LAT, :], pb).astype(BF)
    dp = dot_nt(win_ref[:, :LAT], ga[...])
    delta = jnp.sum(p * dp, 0, keepdims=True)
    ds = (p * (dp - delta) * scale).astype(BF)
    att = dot(win_t[...], ds).astype(BF)
    lat_ref[...] += dot(ds, qf[...])
    lat_ref[:, :LAT] += dot(pb, ga[...])
    mix_r = mix.T
    att_r = att.T
    n = len(masks)
    for which, (left, right) in enumerate(((att[:LAT], qd), (mix, gd))):
        buf[...] = dot(left, right[...]).astype(BF).reshape(buf.shape)
        for k, mask in enumerate(masks):
            piece = buf[meta[2] ^ mask]
            if k < n // 2:
                keep_ref[which, k] = piece
            else:
                send_ref[which, k - n // 2] = piece
    for h in range(2):
        at = slice(h * rows, (h + 1) * rows)
        attn_ref[:, h * VD : (h + 1) * VD] = dot(
            mix_r[at, :], wv_ref[:, h * VD : (h + 1) * VD]
        ).astype(BF)
        qg_ref[:, h * HD : h * HD + NOPE] = dot(
            att_r[at, :LAT], wk_ref[:, h * NOPE : (h + 1) * NOPE]
        ).astype(BF)
        qg_ref[:, h * HD + NOPE : (h + 1) * HD] = att_r[at, LAT:]


def chunk_call(order, shard, first, pairs, meta, query, w_key, w_value, grad, window, lat, outs):
    rows = query.shape[0]
    span = window.shape[0]
    masks = slot_masks(order)
    n = len(masks)
    piece = LAT // n
    full = lambda shape: pl.BlockSpec(shape, lambda i: (0,) * len(shape))
    col = lambda r, c: pl.BlockSpec((r, c), lambda i: (0, i + first))
    own = pl.BlockSpec((2, n // 2, piece, 2 * NOPE), lambda i: (0, 0, 0, i))
    aliases = {}
    extra = []
    if outs is not None:
        extra = list(outs)
        aliases = {7: 0, 8: 1}
    own_shape = jax.ShapeDtypeStruct((2, n // 2, piece, pairs * 2 * NOPE), BF)
    flops = pairs * 4 * rows * LAT * (12 * NOPE + 7 * span)
    return pl.pallas_call(
        functools.partial(body, masks, shard, len(extra)),
        grid=(pairs,),
        in_specs=[
            pl.BlockSpec(memory_space=pltpu.SMEM),
            col(rows, 2 * HD),
            col(LAT, 2 * NOPE),
            col(LAT, 2 * VD),
            col(rows, 2 * VD),
            full(window.shape),
            full(lat.shape),
        ]
        + [pl.BlockSpec(memory_space=pl.ANY)] * len(extra),
        out_specs=[col(rows, 2 * VD), col(rows, 2 * HD), full(lat.shape), own, own],
        out_shape=[
            jax.ShapeDtypeStruct(grad.shape, BF),
            jax.ShapeDtypeStruct(query.shape, BF),
            jax.ShapeDtypeStruct(lat.shape, F32),
            own_shape,
            own_shape,
        ],
        scratch_shapes=[
            pltpu.VMEM((LAT + ROPE, span), BF),
            pltpu.VMEM((span, 2 * rows), F32),
            pltpu.VMEM((2 * rows, LAT + ROPE), BF),
            pltpu.VMEM((2 * rows, LAT), BF),
            pltpu.VMEM((2 * rows, 2 * NOPE), BF),
            pltpu.VMEM((2 * rows, 2 * VD), BF),
            pltpu.VMEM((n, piece, 2 * NOPE), BF),
        ],
        input_output_aliases=aliases,
        cost_estimate=pl.CostEstimate(
            flops=flops, bytes_accessed=pairs * 2_000_000, transcendentals=pairs * 2 * rows * span
        ),
        compiler_params=pltpu.CompilerParams(dimension_semantics=("arbitrary",)),
    )(meta, query, w_key, w_value, grad, window, lat, *extra)


def halve(kept, got, order):
    both = kept.astype(F32) + got.astype(F32)
    half = both.shape[1] // 2
    if half == 0:
        return both
    got = swap(both[:, half:].astype(BF), "ctx", 1 << order[0])
    return halve(both[:, :half], got, order[1:])


def on_device(query, latent, w_key_up, w_value_up, cotangent, window_start):
    rows = query.shape[0]
    heads = w_key_up.shape[1] // NOPE
    n_head = lax.axis_size("head")
    n_ctx = lax.axis_size("ctx")
    shard = latent.shape[0]
    span = (KB + 1) * rows
    cols = LAT + ROPE

    slots = latent[None]
    for b in range(bits_of(n_head)):
        slots = jnp.concatenate([slots, swap(slots, "head", 1 << b)], 0)
    block_rows = slots.reshape(rows, cols)
    window = jnp.concatenate(
        [shifted(block_rows, "ctx", back) for back in range(KB, 0, -1)] + [block_rows], 0
    )
    block = lax.axis_index("ctx")
    meta = jnp.stack(
        [window_start[0] - (block - KB) * rows, lax.axis_index("head"), block]
    ).astype(jnp.int32)

    chunks = min(CHUNKS, heads // 2)
    pairs = heads // 2 // chunks
    lat = jnp.zeros((span, cols), F32)
    outs = None
    summed = []
    for i in range(chunks):
        high = list(range(1, bits_of(n_ctx)))
        turn = i % len(high)
        order = [0] + high[turn:] + high[:turn]
        attn, qg, lat, keep, send = chunk_call(
            order, shard, i * pairs, pairs, meta, query, w_key_up, w_value_up, cotangent, window, lat, outs
        )
        outs = (attn, qg)
        summed.append(halve(keep, swap(send, "ctx", 1), order[1:]))
    key_up_grad = jnp.concatenate([x[0, 0] for x in summed], 1)
    value_up_grad = jnp.concatenate([x[1, 0] for x in summed], 1)

    shares = lat.reshape(KB + 1, n_head, shard, cols)
    for b in reversed(range(bits_of(n_head))):
        half = 1 << b
        shares = shares[:, :half] + swap(shares[:, half:].astype(BF), "head", half).astype(F32)
    shares = shares[:, 0]
    latent_grad = shares[KB]
    for back in range(1, KB + 1):
        latent_grad = latent_grad + shifted(shares[KB - back].astype(BF), "ctx", -back).astype(F32)
    return (attn, qg, latent_grad, key_up_grad, value_up_grad)


def solution(mesh):
    return jax.shard_map(
        on_device,
        mesh=mesh,
        in_specs=(
            P("ctx", "head"),
            P(("ctx", "head"), None),
            P(None, "head"),
            P(None, "head"),
            P("ctx", "head"),
            P("ctx"),
        ),
        out_specs=(
            P("ctx", "head"),
            P("ctx", "head"),
            P(("ctx", "head"), None),
            P("ctx", "head"),
            P("ctx", "head"),
        ),
        check_vma=False,
    )
```
